8 devices in a mesh: dp: 2 (over z, y), stage: 2 (over x), tp: 2 (over core).
Axes of the slice: x: 2, y: 2, z: 1, core: 2. Of those that a mesh axis runs over, the one named last changes fastest.
Arguments:
- act_in: bfloat16 [2, 24, 28, 28, 512], P('stage', ('dp', 'tp'))
- w_conv: bfloat16 [2, 3, 3, 512, 512], P('stage', None, None, 'tp')
- w_short: bfloat16 [2, 512, 512], P('stage', 'tp')
- gamma: float32 [2, 512], P('stage', 'tp')
- beta: float32 [2, 512], P('stage', 'tp')
- gamma_s: float32 [2, 512], P('stage', 'tp')
- grad_z: bfloat16 [2, 24, 28, 28, 512], P('stage', 'dp', None, None, 'tp')
Outputs:
- output 1: bfloat16 [2, 24, 28, 28, 512], P('stage', 'dp', None, None, 'tp')
- output 2: bfloat16 [2, 24, 28, 28, 512], P('stage', ('dp', 'tp'))
- output 3: float32 [2, 3, 3, 512, 512], P('stage', None, None, 'tp')
- output 4: float32 [2, 512, 512], P('stage', 'tp')
All inputs are finite; a program needn't handle non-finite values.
Results may differ from the reference program's by a relative error of at most 0.00383.
Values are sent between devices in bfloat16 or wider.
A program may use at most 1 GiB of HBM per device.

```python
import jax
import jax.numpy as jnp
from jax import lax

NUM_STAGES = 2
BATCH_ALL = 24
BLOCK_IMGS = 6
IMG_HEIGHT = 28
IMG_WIDTH = 28
CH_IN = 512
CH_OUT = 512


def place_slot(array_in, slot_index):
    pad_before = jnp.zeros((slot_index,) + array_in.shape, array_in.dtype)
    pad_after = jnp.zeros((NUM_STAGES - slot_index - 1,) + array_in.shape, array_in.dtype)
    return jnp.concatenate([pad_before, array_in[None], pad_after], axis=0)


def setup_inputs(seed: int = 0) -> dict:
    key_list = jax.random.split(jax.random.key(seed), 7)
    act_draw = jax.random.normal(key_list[0], (BATCH_ALL, IMG_HEIGHT, IMG_WIDTH, CH_IN), jnp.float32)
    conv_draw = jax.random.normal(key_list[1], (3, 3, CH_IN, CH_OUT), jnp.float32) * (9 * CH_IN) ** -0.5
    short_draw = jax.random.normal(key_list[2], (CH_IN, CH_OUT), jnp.float32) * CH_IN ** -0.5
    gamma_draw = jax.random.uniform(key_list[3], (CH_OUT,), jnp.float32, 0.5, 1.5)
    beta_draw = 0.5 * jax.random.normal(key_list[4], (CH_OUT,), jnp.float32)
    gamma_s_draw = jax.random.uniform(key_list[5], (CH_OUT,), jnp.float32, 0.5, 1.5)
    grad_draw = jax.random.normal(key_list[6], (BATCH_ALL, IMG_HEIGHT, IMG_WIDTH, CH_OUT), jnp.float32)
    return {
        "act_in": place_slot(act_draw.astype(jnp.bfloat16), 0),
        "w_conv": place_slot(conv_draw.astype(jnp.bfloat16), 1),
        "w_short": place_slot(short_draw.astype(jnp.bfloat16), 1),
        "gamma": place_slot(gamma_draw, 1),
        "beta": place_slot(beta_draw, 1),
        "gamma_s": place_slot(gamma_s_draw, 1),
        "grad_z": place_slot(grad_draw.astype(jnp.bfloat16), 1),
    }


def reference(act_in, w_conv, w_short, gamma, beta, gamma_s, grad_z):
    kernel = w_conv[1].astype(jnp.float32)
    short_w = w_short[1].astype(jnp.float32)
    scale_main = gamma[1]
    shift_main = beta[1]
    scale_short = gamma_s[1]
    num_blocks = BATCH_ALL // BLOCK_IMGS
    act_blocks = act_in[0].reshape(num_blocks, BLOCK_IMGS, IMG_HEIGHT, IMG_WIDTH, CH_IN)
    grad_blocks = grad_z[1].reshape(num_blocks, BLOCK_IMGS, IMG_HEIGHT, IMG_WIDTH, CH_OUT)

    def linear_part(images, conv_w, proj_w):
        pre_act = lax.conv_general_dilated(images, conv_w, (1, 1), "SAME", dimension_numbers=("NHWC", "HWIO", "NHWC"))
        short_out = jnp.einsum("nhwc,co->nhwo", images, proj_w)
        return pre_act, short_out

    def block_step(acc_pair, block_in):
        act_blk, grad_blk = block_in
        (pre_act, short_out), pull_back = jax.vjp(linear_part, act_blk.astype(jnp.float32), kernel, short_w)
        mixed_sum = pre_act * scale_main + shift_main + short_out * scale_short
        z_blk = jnp.maximum(mixed_sum, 0.0).astype(jnp.bfloat16)
        mask_pos = mixed_sum > 0.0
        grad_wide = grad_blk.astype(jnp.float32)
        g_main = jnp.where(mask_pos, grad_wide * scale_main, 0.0).astype(jnp.bfloat16)
        g_short = jnp.where(mask_pos, grad_wide * scale_short, 0.0).astype(jnp.bfloat16)
        grad_images, grad_conv, grad_proj = pull_back((g_main.astype(jnp.float32), g_short.astype(jnp.float32)))
        new_acc = (acc_pair[0] + grad_conv, acc_pair[1] + grad_proj)
        return new_acc, (z_blk, grad_images.astype(jnp.bfloat16))

    acc_init = (jnp.zeros((3, 3, CH_IN, CH_OUT), jnp.float32), jnp.zeros((CH_IN, CH_OUT), jnp.float32))
    (dw_sum, dws_sum), (z_blocks, dx_blocks) = lax.scan(block_step, acc_init, (act_blocks, grad_blocks))
    z_all = z_blocks.reshape(BATCH_ALL, IMG_HEIGHT, IMG_WIDTH, CH_OUT)
    dx_all = dx_blocks.reshape(BATCH_ALL, IMG_HEIGHT, IMG_WIDTH, CH_IN)
    return (place_slot(z_all, 1), place_slot(dx_all, 0), place_slot(dw_sum, 1), place_slot(dws_sum, 1))
```

```python
import functools

import jax
import jax.numpy as jnp
from jax import lax
from jax.experimental import pallas as pl
from jax.experimental.pallas import tpu as pltpu
from jax.sharding import PartitionSpec as P

MESH = pl.DeviceIdType.MESH
F32, BF16 = jnp.float32, jnp.bfloat16
NI = 6
PITCH = 32
ROWS = 28 * PITCH
HALO = PITCH
C = 512
HC = 256
CH = 448
EC = 128
NMSG = 10
DETOUR = (0, 2, 4, 6)
DIRECT = (1, 3, 5, 7, 8, 9)


def rcopy(src, dst, send, recv, dev):
    return pltpu.make_async_remote_copy(src_ref=src, dst_ref=dst, send_sem=send, recv_sem=recv, device_id=dev, device_id_type=MESH)


def dot(a, b):
    return jnp.dot(a, b, preferred_element_type=F32)


def body(x_in, dz_in, w_in, ws_in, vec_in, z_out, dx_out, dw_out,
         xr, dzv, wc, wt, sw, st, acc, tpr, dpr, xcat, gcat, gs, xt, vec,
         xs, xrv, dzl, dzs, dzr, wl, wsd, wr, vl, vs, vr, zl, zs, zr,
         dxs, dxr, ts, tr, ys, yr, ras, rar, rbs, rbr, ol):
    tp = lax.axis_index("tp")
    stage = lax.axis_index("stage")
    dp = lax.axis_index("dp")
    p_x = {"stage": 1 - stage}
    p_t = {"tp": 1 - tp}
    p_d = {"dp": 1 - dp}

    barrier = pltpu.get_barrier_semaphore()
    for dev in (p_x, p_t, p_d):
        pl.semaphore_signal(barrier, inc=1, device_id=dev, device_id_type=MESH)
    pl.semaphore_wait(barrier, 3)

    def x_copy(k):
        return rcopy(x_in.at[k], xr.at[k], xs.at[k], xrv.at[k], p_x)

    def dx_copy(k):
        return rcopy(xr.at[k], dx_out.at[k], dxs.at[k], dxr.at[k], p_x)

    def relay_a(n):
        m = DETOUR[n]
        return rcopy(acc.at[m, pl.ds(pl.multiple_of(tp * HC, HC), HC)], tpr.at[n], ys.at[m], rar.at[n], p_x)

    def relay_b(n):
        return rcopy(tpr.at[n], dpr.at[n], ras.at[n], rbr.at[n], p_d)

    def relay_c(n):
        m = DETOUR[n]
        return rcopy(dpr.at[n], dpr.at[m], rbs.at[n], yr.at[m], p_x)

    @pl.when(stage == 0)
    def _():
        x_copy(0).start()
        x_copy(1).start()
        for k in range(2, NI):
            x_copy(k - 2).wait_send()
            x_copy(k).start()
        x_copy(NI - 2).wait_send()
        x_copy(NI - 1).wait_send()
        nd = len(DETOUR)
        for n in range(nd + 1):
            if n < nd:
                relay_a(n).wait_recv()
                relay_b(n).start()
            if n > 0:
                relay_b(n - 1).wait_recv()
                relay_c(n - 1).start()
        for n in range(nd):
            relay_b(n).wait_send()
            relay_c(n).wait_send()
        for k in range(NI):
            dx_copy(k).wait_recv()

    @pl.when(stage == 1)
    def _():
        lanes = pl.ds(pl.multiple_of(tp * HC, HC), HC)
        other = pl.ds(pl.multiple_of((1 - tp) * HC, HC), HC)

        def dz_local(k):
            return pltpu.make_async_copy(dz_in.at[tp * NI + k], dzv.at[k, :, lanes], dzl.at[k])

        def dz_remote(k):
            return rcopy(dz_in.at[(1 - tp) * NI + k], dzv.at[k, :, lanes], dzs.at[k], dzr.at[k], p_t)

        def w_dst(m):
            if m == 9:
                return sw.at[lanes]
            i, j = divmod(m, 3)
            return wc.at[i, pl.ds(pl.multiple_of(j * C + tp * HC, HC), HC)]

        def w_src(m):
            return ws_in if m == 9 else w_in.at[m]

        def w_local(m):
            return pltpu.make_async_copy(w_src(m), w_dst(m), wl.at[m])

        def w_remote(m):
            return rcopy(w_src(m), w_dst(m), wsd.at[m], wr.at[m], p_t)

        def v_local():
            return pltpu.make_async_copy(vec_in, vec.at[:, lanes], vl.at[0])

        def v_remote():
            return rcopy(vec_in, vec.at[:, lanes], vs.at[0], vr.at[0], p_t)

        def z_local(k):
            return pltpu.make_async_copy(dzv.at[k, :, lanes], z_out.at[tp * NI + k], zl.at[k])

        def z_remote(k):
            return rcopy(dzv.at[k, :, other], z_out.at[tp * NI + k], zs.at[k], zr.at[k], p_t)

        def t_copy(m):
            return rcopy(acc.at[m, other], tpr.at[m], ts.at[m], tr.at[m], p_t)

        def y_copy(m):
            return rcopy(acc.at[m, lanes], dpr.at[m], ys.at[m], yr.at[m], p_d)

        def out_copy(m):
            return pltpu.make_async_copy(tpr.at[m], dw_out.at[m], ol.at[m])

        for m in range(NMSG):
            w_local(m).start()
            w_remote(m).start()
        v_local().start()
        v_remote().start()

        @pl.loop(0, NI)
        def _(k):
            dz_local(k).start()
            dz_remote(k).start()

        @pl.loop(0, NMSG)
        def _(m):
            acc[m] = jnp.zeros((C, C), F32)

        for ref in (xcat, gcat):
            ref[0:HALO] = jnp.zeros((HALO, 3 * C), BF16)
            ref[HALO + ROWS:] = jnp.zeros((HALO, 3 * C), BF16)
        for m in range(NMSG):
            w_local(m).wait()
            w_remote(m).wait()
        v_local().wait()
        v_remote().wait()
        st[...] = sw[...].T

        @pl.loop(0, 3)
        def _(i):
            for j in range(3):
                wt[i, j * C:(j + 1) * C] = wc[i, j * C:(j + 1) * C].T

        @pl.loop(0, NI)
        def _(k):
            x_copy(k).wait_recv()
            for e in range(ROWS // EC):
                xv = xr[k, e * EC:(e + 1) * EC]
                xf = xv.astype(F32)
                dst = slice(HALO + e * EC, HALO + (e + 1) * EC)
                xcat[dst, C:2 * C] = xv
                xcat[dst, 0:C] = pltpu.roll(xf, 1, 0).astype(BF16)
                xcat[dst, 2 * C:] = pltpu.roll(xf, EC - 1, 0).astype(BF16)
            dz_local(k).wait()
            dz_remote(k).wait()
            for r in range(0, ROWS, CH):
                pre = dot(xcat[r:r + CH], wc[0]) + dot(xcat[r + HALO:r + HALO + CH], wc[1]) + dot(xcat[r + 2 * HALO:r + 2 * HALO + CH], wc[2])
                short = dot(xcat[r + HALO:r + HALO + CH, C:2 * C], sw[...])
                u = pre * vec[0:1] + vec[1:2] + short * vec[2:3]
                dz = dzv[k, r:r + CH].astype(F32)
                dzv[k, r:r + CH] = jnp.maximum(u, 0.0).astype(BF16)
                g = jnp.where(u > 0.0, dz * vec[0:1], 0.0)
                gs[r:r + CH] = jnp.where(u > 0.0, dz * vec[2:3], 0.0).astype(BF16)
                dst = slice(HALO + r, HALO + r + CH)
                gcat[dst, 0:C] = pltpu.roll(g, CH - 1, 0).astype(BF16)
                gcat[dst, C:2 * C] = g.astype(BF16)
                gcat[dst, 2 * C:] = pltpu.roll(g, 1, 0).astype(BF16)
            z_local(k).start()
            z_remote(k).start()

            for i in range(3):
                xt[i] = xcat[i * HALO:i * HALO + ROWS, C:2 * C].T
            for i in range(3):
                for j in range(3):
                    acc[3 * i + j] += dot(xt[i], gcat[HALO:HALO + ROWS, j * C:(j + 1) * C])
            acc[9] += dot(xt[1], gs[...])

            @pl.when(k == NI - 1)
            def _():
                for m in range(NMSG):
                    t_copy(m).start()
                for m in range(NMSG):
                    t_copy(m).wait_recv()
                    acc[m, lanes] = acc[m, lanes] + tpr[m]
                    if m in DETOUR:
                        relay_a(DETOUR.index(m)).start()
                    else:
                        y_copy(m).start()

            for r in range(0, ROWS, CH):
                dx = dot(gcat[r + 2 * HALO:r + 2 * HALO + CH], wt[0]) + dot(gcat[r + HALO:r + HALO + CH], wt[1]) + dot(gcat[r:r + CH], wt[2]) + dot(gs[r:r + CH], st[...])
                xr[k, r:r + CH] = dx.astype(BF16)
            dx_copy(k).start()

        for m in DIRECT + DETOUR:
            y_copy(m).wait_recv()
            tpr[m] = acc[m, lanes] + dpr[m]
            out_copy(m).start()

        @pl.loop(0, NMSG)
        def _(m):
            t_copy(m).wait_send()
            y_copy(m).wait_send()
            out_copy(m).wait()

        @pl.loop(0, NI)
        def _(k):
            z_local(k).wait()
            z_remote(k).wait()
            dx_copy(k).wait_send()


def block(x_pad, dz_pad, w, ws, vecs):
    any_spec = pl.BlockSpec(memory_space=pl.ANY)
    dma = lambda n: pltpu.SemaphoreType.DMA((n,))
    nd = len(DETOUR)
    return pl.pallas_call(
        body,
        out_shape=(
            jax.ShapeDtypeStruct((2 * NI, ROWS, HC), BF16),
            jax.ShapeDtypeStruct((NI, ROWS, C), BF16),
            jax.ShapeDtypeStruct((NMSG, HC, C), F32),
        ),
        in_specs=[any_spec] * 5,
        out_specs=(any_spec,) * 3,
        scratch_shapes=[
            pltpu.VMEM((NI, ROWS, C), BF16),
            pltpu.VMEM((NI, ROWS, C), BF16),
            pltpu.VMEM((3, 3 * C, C), BF16),
            pltpu.VMEM((3, 3 * C, C), BF16),
            pltpu.VMEM((C, C), BF16),
            pltpu.VMEM((C, C), BF16),
            pltpu.VMEM((NMSG, C, C), F32),
            pltpu.VMEM((NMSG, HC, C), F32),
            pltpu.VMEM((NMSG, HC, C), F32),
            pltpu.VMEM((ROWS + 2 * HALO, 3 * C), BF16),
            pltpu.VMEM((ROWS + 2 * HALO, 3 * C), BF16),
            pltpu.VMEM((ROWS, C), BF16),
            pltpu.VMEM((3, C, ROWS), BF16),
            pltpu.VMEM((8, C), F32),
            dma(NI), dma(NI), dma(NI), dma(NI), dma(NI), dma(NMSG), dma(NMSG), dma(NMSG), dma(1), dma(1), dma(1), dma(NI), dma(NI), dma(NI),
            dma(NI), dma(NI), dma(NMSG), dma(NMSG), dma(NMSG), dma(NMSG), dma(nd), dma(nd), dma(nd), dma(nd), dma(NMSG),
        ],
        compiler_params=pltpu.CompilerParams(collective_id=0, has_side_effects=True, vmem_limit_bytes=67043328),
        name="conv_block",
    )(x_pad, dz_pad, w, ws, vecs)


def solution(mesh):
    act_spec = P("stage", ("dp", "tp"), None, None, None)
    kernel_spec = P("stage", None, None, "tp", None)
    short_spec = P("stage", "tp", None)
    vec_spec = P("stage", "tp")
    grad_spec = P("stage", "dp", None, None, "tp")

    def device_step(act_in, w_conv, w_short, gamma, beta, gamma_s, grad_z):
        stage = lax.axis_index("stage")
        widen = lambda a: jnp.pad(a, ((0, 0), (0, 0), (0, PITCH - 28), (0, 0))).reshape(a.shape[0], ROWS, a.shape[3])
        narrow = lambda a: a.reshape(a.shape[0], 28, PITCH, a.shape[2])[:, :, :28]
        vecs = jnp.concatenate([gamma, beta, gamma_s, jnp.zeros((5, HC), F32)], axis=0)
        z, dx, dw = block(widen(act_in[0]), widen(grad_z[0]), w_conv.reshape(9, HC, C), w_short[0], vecs)
        z = jnp.where(stage == 1, narrow(z), jnp.zeros((), BF16))
        dx = jnp.where(stage == 0, narrow(dx), jnp.zeros((), BF16))
        dw = jnp.where(stage == 1, dw, 0.0)
        return z[None], dx[None], dw[:9].reshape(1, 3, 3, HC, C), dw[9][None]

    return jax.shard_map(device_step, mesh=mesh, in_specs=(act_spec, kernel_spec, short_spec, vec_spec, vec_spec, vec_spec, grad_spec), out_specs=(grad_spec, act_spec, kernel_spec, short_spec), check_vma=False)
```

```python
import jax
import jax.numpy as jnp
from jax import lax
from jax.experimental import pallas as pl
from jax.experimental.pallas import tpu as pltpu
from jax.sharding import PartitionSpec as P

MESH = pl.DeviceIdType.MESH
F32, BF16 = jnp.float32, jnp.bfloat16
NI = 6
SIDE = 28
PITCH = 32
ROWS = SIDE * PITCH
PIX = SIDE * SIDE
HALO = PITCH
C = 512
HC = 256
BLK, PBLK = 4 * PITCH, 4 * SIDE
CHUNKS = ((0, 512), (512, 384))
DXCHUNKS = ((0, 384), (384, 512))
NTAP = 10
UNIT = 64
NU = HC // UNIT
RELAYED = tuple((m, s) for m in range(9) for s in range(2))[:18]
STRAIGHT = tuple((m, s) for m in range(NTAP) for s in range(NU) if (m, s) not in RELAYED)
ARRIVAL = sorted([(i + 1, u) for i, u in enumerate(STRAIGHT)] + [(i + 5.5, u) for i, u in enumerate(RELAYED)])
SPLIT = 5


def rcopy(src, dst, send, recv, dev):
    return pltpu.make_async_remote_copy(src_ref=src, dst_ref=dst, send_sem=send, recv_sem=recv, device_id=dev, device_id_type=MESH)


def dot(a, b):
    return jnp.dot(a, b, preferred_element_type=F32)


def body(x_in, dz_in, w_in, ws_in, gam_in, bet_in, gas_in, z_out, dx_out, dw_out, ds_out,
         xr, dzv, wc, wt, sw, st, acc, tpr, dpr, xcat, gcat, gs, xt, gam, bet, gas, xraw, dzraw, dzt, widen, pack,
         xs, xrv, xl, dzl, dzs, dzr, wl, wsd, wr, vl, vs, vr, zl, zs, zr,
         dxs, dxr, dxo, ts, tr, ys, yr, ras, rar, rbs, rbr, ol):
    tp = lax.axis_index("tp")
    stage = lax.axis_index("stage")
    p_x = {"stage": 1 - stage}
    p_t = {"tp": 1 - tp}
    p_d = {"dp": 1 - lax.axis_index("dp")}

    def load_part(k):
        x_load(k).wait()
        for h in range(SIDE):
            gs[h * PITCH:h * PITCH + SIDE] = xraw[k % 2, h]
        if k + 2 < NI:
            x_load(k + 2).start()

    def pack_part(k, p):
        for b in range(SPLIT) if p == 0 else range(SPLIT, SIDE // 4):
            xr[k, b * PBLK:(b + 1) * PBLK] = dot(pack[...], gs[b * BLK:(b + 1) * BLK]).astype(BF16)

    barrier = pltpu.get_barrier_semaphore()
    for dev in (p_x, p_t, p_d):
        pl.semaphore_signal(barrier, inc=1, device_id=dev, device_id_type=MESH)

    def select(shape, padded_axis):
        wide = lax.broadcasted_iota(jnp.int32, shape, padded_axis)
        slim = lax.broadcasted_iota(jnp.int32, shape, 1 - padded_axis)
        col = wide & (PITCH - 1)
        hit = (slim == (wide >> 5) * SIDE + col) & (col < SIDE)
        return jnp.where(hit, 1.0, 0.0).astype(BF16)


    def x_copy(k, p):
        at = slice(0, SPLIT * PBLK) if p == 0 else slice(SPLIT * PBLK, PIX)
        return rcopy(xr.at[k, at], xr.at[k, at], xs.at[k, p], xrv.at[k, p], p_x)

    def x_load(k):
        return pltpu.make_async_copy(x_in.at[k], xraw.at[k % 2], xl.at[k])

    def dx_copy(k, c, h):
        r, n = DXCHUNKS[c]
        at = slice(r // PITCH * SIDE, (r + n) // PITCH * SIDE)
        return rcopy(xr.at[k, at, h * HC:(h + 1) * HC], dzv.at[k, h, at], dxs.at[k, c, h], dxr.at[k, c, h], p_x)

    def unit_rows(u):
        return pl.ds(pl.multiple_of(tp * HC + u[1] * UNIT, UNIT), UNIT)

    def part(ref, u):
        return ref.at[u[0], u[1] * UNIT:(u[1] + 1) * UNIT]

    def held(ref, n):
        return part(ref, divmod(n, NU))

    def relay_a(n):
        m, s = RELAYED[n]
        return rcopy(acc.at[m, unit_rows((m, s))], held(tpr, n), ys.at[m, s], rar.at[n], p_x)

    def relay_b(n):
        return rcopy(held(tpr, n), held(dpr, n), ras.at[n], rbr.at[n], p_d)

    def relay_c(n):
        m, s = RELAYED[n]
        return rcopy(held(dpr, n), part(dpr, (m, s)), rbs.at[n], yr.at[m, s], p_x)

    widen[...] = select((BLK, PBLK), 0)
    pack[...] = select((PBLK, BLK), 1)

    @pl.when(stage == 0)
    def _():
        x_load(0).start()
        x_load(1).start()
        gs[...] = jnp.zeros((ROWS, C), BF16)
        load_part(0)
        pack_part(0, 0)
        pack_part(0, 1)

    pl.semaphore_wait(barrier, 3)

    @pl.when(stage == 0)
    def _():
        def dx_store(k):
            return pltpu.make_async_copy(xraw.at[k % 2], dx_out.at[k], dxo.at[k])

        x_copy(0, 0).start()
        x_copy(0, 1).start()
        for k in range(1, NI):
            load_part(k)
            pack_part(k, 0)
            if k > 1:
                x_copy(k - 2, 0).wait_send()
                x_copy(k - 2, 1).wait_send()
            x_copy(k, 0).start()
            pack_part(k, 1)
            x_copy(k, 1).start()
        for k in range(NI - 2, NI):
            x_copy(k, 0).wait_send()
            x_copy(k, 1).wait_send()

        def take_dx(k):
            for c in range(2):
                for h in range(2):
                    dx_copy(k, c, h).wait_recv()
            if k > 1:
                dx_store(k - 2).wait()
            for b in range(SIDE // 4):
                for h in range(2):
                    wide = dot(widen[...], dzv[k, h, b * PBLK:(b + 1) * PBLK]).astype(BF16)
                    for r in range(4):
                        xraw[k % 2, 4 * b + r, :, h * HC:(h + 1) * HC] = wide[r * PITCH:r * PITCH + SIDE]
            dx_store(k).start()

        for k in range(NI - 1):
            take_dx(k)
        nr = len(RELAYED)
        for n in range(nr + 1):
            if n < nr:
                relay_a(n).wait_recv()
                relay_b(n).start()
            if n > 0:
                relay_b(n - 1).wait_recv()
                relay_c(n - 1).start()
        take_dx(NI - 1)
        for n in range(nr):
            relay_b(n).wait_send()
            relay_c(n).wait_send()
        dx_store(NI - 2).wait()
        dx_store(NI - 1).wait()

    @pl.when(stage == 1)
    def _():
        lanes = pl.ds(pl.multiple_of(tp * HC, HC), HC)
        other = pl.ds(pl.multiple_of((1 - tp) * HC, HC), HC)

        def dz_load(k, q):
            img = (tp if q == 0 else 1 - tp) * NI + k
            return pltpu.make_async_copy(dz_in.at[img], dzraw.at[lax.rem(k, 2), q], dzl.at[k, q])

        def dz_send(k):
            return rcopy(dzt.at[lax.rem(k, 2)], dzv.at[k, tp], dzs.at[k], dzr.at[k], p_t)

        def w_dst(m):
            if m == 9:
                return sw.at[lanes]
            i, j = divmod(m, 3)
            return wc.at[i, pl.ds(pl.multiple_of(j * C + tp * HC, HC), HC)]

        def w_src(m):
            return ws_in if m == 9 else w_in.at[m]

        def w_local(m):
            return pltpu.make_async_copy(w_src(m), w_dst(m), wl.at[m])

        def w_remote(m):
            return rcopy(w_src(m), w_dst(m), wsd.at[m], wr.at[m], p_t)

        vecs = ((gam_in, gam), (bet_in, bet), (gas_in, gas))

        def v_local(i):
            return pltpu.make_async_copy(vecs[i][0], vecs[i][1].at[:, lanes], vl.at[i])

        def v_remote(i):
            return rcopy(vecs[i][0], vecs[i][1].at[:, lanes], vs.at[i], vr.at[i], p_t)

        def z_local(k):
            return pltpu.make_async_copy(dzraw.at[lax.rem(k, 2), tp], z_out.at[tp * NI + k], zl.at[k])

        def z_remote(k):
            return rcopy(dzraw.at[lax.rem(k, 2), 1 - tp], z_out.at[tp * NI + k], zs.at[k], zr.at[k], p_t)

        def t_copy(m):
            return rcopy(acc.at[m, other], tpr.at[m], ts.at[m], tr.at[m], p_t)

        def y_copy(u):
            return rcopy(acc.at[u[0], unit_rows(u)], part(dpr, u), ys.at[u[0], u[1]], yr.at[u[0], u[1]], p_d)

        def out_copy(u):
            m, s = u
            rows = slice(s * UNIT, (s + 1) * UNIT)
            dst = ds_out.at[rows] if m == 9 else dw_out.at[m, rows]
            return pltpu.make_async_copy(part(tpr, u), dst, ol.at[m, s])

        for k in range(2):
            for q in range(2):
                dz_load(k, q).start()
        for m in range(NTAP):
            w_local(m).start()
            w_remote(m).start()
        for i in range(3):
            v_local(i).start()
            v_remote(i).start()

        zero = jnp.zeros((ROWS, HC), BF16)
        for q in range(2):
            dzt[q] = zero

        @pl.loop(0, NI)
        def _(k):
            dzv[k, tp] = zero
            for q in range(2):
                dz_load(k, q).wait()

            @pl.when(k >= 2)
            def _():
                dz_send(k - 2).wait_send()

            slot = lax.rem(k, 2)
            for h in range(SIDE):
                dzv[k, tp, h * PITCH:h * PITCH + SIDE] = dzraw[slot, 0, h]
                dzt[slot, h * PITCH:h * PITCH + SIDE] = dzraw[slot, 1, h]
            dz_send(k).start()

            @pl.when(k < NI - 2)
            def _():
                for q in range(2):
                    dz_load(k + 2, q).start()

        @pl.loop(0, NTAP)
        def _(m):
            acc[m] = jnp.zeros((C, C), F32)

        for ref in (xcat, gcat):
            ref[0:HALO] = jnp.zeros((HALO, 3 * C), BF16)
            ref[HALO + ROWS:] = jnp.zeros((HALO, 3 * C), BF16)
        for m in range(NTAP):
            w_local(m).wait()
            w_remote(m).wait()
        for i in range(3):
            v_local(i).wait()
            v_remote(i).wait()
        st[...] = sw[...].T

        @pl.loop(0, 3)
        def _(i):
            for j in range(3):
                wt[i, j * C:(j + 1) * C] = wc[i, j * C:(j + 1) * C].T

        @pl.loop(0, 2)
        def _(k):
            dz_send(NI - 2 + k).wait_send()

        def pass_on(m):
            t_copy(m).wait_recv()
            for s in range(NU):
                u = (m, s)
                rows = unit_rows(u)
                acc[m, rows] = acc[m, rows] + tpr[m, s * UNIT:(s + 1) * UNIT]
                if u in RELAYED:
                    relay_a(RELAYED.index(u)).start()
                else:
                    y_copy(u).start()

        def forward(k, blocks, r, n):
            for b in blocks:
                xf = dot(widen[...], xr[k, b * PBLK:(b + 1) * PBLK])
                dst = slice(HALO + b * BLK, HALO + (b + 1) * BLK)
                xcat[dst, C:2 * C] = xf.astype(BF16)
                xcat[dst, 0:C] = pltpu.roll(xf, 1, 0).astype(BF16)
                xcat[dst, 2 * C:] = pltpu.roll(xf, BLK - 1, 0).astype(BF16)
            pre = dot(xcat[r:r + n], wc[0]) + dot(xcat[r + HALO:r + HALO + n], wc[1]) + dot(xcat[r + 2 * HALO:r + 2 * HALO + n], wc[2])
            short = dot(xcat[r + HALO:r + HALO + n, C:2 * C], sw[...])
            u = pre * gam[...] + bet[...] + short * gas[...]
            z = jnp.maximum(u, 0.0).astype(BF16)
            for h in range(n // PITCH):
                for q in range(2):
                    dzraw[lax.rem(k, 2), q, r // PITCH + h] = z[h * PITCH:h * PITCH + SIDE, q * HC:(q + 1) * HC]
            dz = jnp.concatenate([dzv[k, 0, r:r + n], dzv[k, 1, r:r + n]], axis=1).astype(F32)
            g = jnp.where(u > 0.0, dz * gam[...], 0.0)
            gs[r:r + n] = jnp.where(u > 0.0, dz * gas[...], 0.0).astype(BF16)
            dst = slice(HALO + r, HALO + r + n)
            gcat[dst, 0:C] = pltpu.roll(g, n - 1, 0).astype(BF16)
            gcat[dst, C:2 * C] = g.astype(BF16)
            gcat[dst, 2 * C:] = pltpu.roll(g, 1, 0).astype(BF16)

        def image(k, last):
            def free_slot():
                z_local(k - 2).wait()
                z_remote(k - 2).wait_send()

            free_slot() if last else pl.when(k >= 2)(free_slot)
            dz_send(k).wait_recv()
            x_copy(k, 0).wait_recv()
            forward(k, range(SPLIT), *CHUNKS[0])

            def input_part(c):
                r, n = DXCHUNKS[c]
                dx = dot(gcat[r + 2 * HALO:r + 2 * HALO + n], wt[0]) + dot(gcat[r + HALO:r + HALO + n], wt[1]) + dot(gcat[r:r + n], wt[2]) + dot(gs[r:r + n], st[...])
                dx = dx.astype(BF16)
                for b in range(n // BLK):
                    at = (r // BLK + b) * PBLK
                    xr[k, at:at + PBLK] = dot(pack[...], dx[b * BLK:(b + 1) * BLK]).astype(BF16)
                for h in range(2):
                    dx_copy(k, c, h).start()

            input_part(0)
            x_copy(k, 1).wait_recv()
            forward(k, range(SPLIT, SIDE // 4), *CHUNKS[1])
            z_local(k).start()
            z_remote(k).start()

            def weight_part():
                xt[...] = xcat[HALO:HALO + ROWS, C:2 * C].T
                for m in range(NTAP):
                    if m == 9:
                        acc[9] += dot(xt[...], gs[...])
                    else:
                        i, j = divmod(m, 3)
                        at = (2 - i) * HALO
                        acc[m] += dot(xt[...], gcat[at:at + ROWS, j * C:(j + 1) * C])
                    if last:
                        t_copy(m).start()
                        if m >= 2:
                            pass_on(m - 2)
                if last:
                    pass_on(NTAP - 2)
                    pass_on(NTAP - 1)

            if last:
                weight_part()
                input_part(1)
            else:
                input_part(1)
                weight_part()

        @pl.loop(0, NI - 1)
        def _(k):
            image(k, False)

        image(NI - 1, True)

        for _, u in ARRIVAL:
            y_copy(u).wait_recv()
            m, s = u
            tpr[m, s * UNIT:(s + 1) * UNIT] = acc[m, unit_rows(u)] + part(dpr, u)[...]
            out_copy(u).start()

        for m in range(NTAP):
            t_copy(m).wait_send()
            for s in range(NU):
                y_copy((m, s)).wait_send()
                out_copy((m, s)).wait()

        for k in range(NI - 2, NI):
            z_local(k).wait()
            z_remote(k).wait_send()
        for k in range(NI):
            z_remote(k).wait_recv()
            for c in range(2):
                for h in range(2):
                    dx_copy(k, c, h).wait_send()


def finish_body(z_in, dx_in, dw_in, ds_in, z_out, dx_out, dw_out, ds_out, zb, dxb, dwb, dsb, z0, dx0, dw0, sems):
    stage = lax.axis_index("stage")
    groups = ((z_in, zb, z_out, z0, 2 * NI, 1), (dx_in, dxb, dx_out, dx0, NI, 0), (dw_in, dwb, dw_out, dw0, 9, 1), (ds_in, dsb, ds_out, dw0, 1, 1))

    def run(here):
        def pick(ref, k):
            return ref.at[k] if len(ref.shape) > 2 else ref

        ins, outs, n = [], [], 0
        for src, buf, dst, nil, count, owner in groups:
            for k in range(count):
                if owner == here:
                    ins.append(pltpu.make_async_copy(pick(src, k), pick(buf, k), sems.at[0, n]))
                    outs.append(pltpu.make_async_copy(pick(buf, k), pick(dst, k), sems.at[1, n]))
                else:
                    outs.append(pltpu.make_async_copy(nil, pick(dst, k), sems.at[1, n]))
                    ins.append(None)
                n += 1
        for c in ins:
            if c is not None:
                c.start()
        if here == 0:
            z0[...] = jnp.zeros(z0.shape, z0.dtype)
            dw0[...] = jnp.zeros(dw0.shape, dw0.dtype)
        else:
            dx0[...] = jnp.zeros(dx0.shape, dx0.dtype)
        for c, o in zip(ins, outs):
            if c is None:
                o.start()
        for c, o in zip(ins, outs):
            if c is not None:
                c.wait()
                o.start()
        for o in outs:
            o.wait()

    for here in range(2):
        pl.when(stage == here)(lambda here=here: run(here))


def finish(z, dx, dw, ds):
    any_spec = pl.BlockSpec(memory_space=pl.ANY)
    total = 2 * NI + NI + 9 + 1
    return pl.pallas_call(
        finish_body,
        out_shape=tuple(jax.ShapeDtypeStruct(a.shape, a.dtype) for a in (z, dx, dw, ds)),
        in_specs=[any_spec] * 4,
        out_specs=(any_spec,) * 4,
        scratch_shapes=[pltpu.VMEM(a.shape, a.dtype) for a in (z, dx, dw, ds)]
        + [pltpu.VMEM(z.shape[1:], z.dtype), pltpu.VMEM(dx.shape[1:], dx.dtype), pltpu.VMEM(ds.shape, ds.dtype), pltpu.SemaphoreType.DMA((2, total))],
        compiler_params=pltpu.CompilerParams(vmem_limit_bytes=67043328),
        name="finish",
    )(z, dx, dw, ds)


def block(x, dz, w, ws, gamma, beta, gamma_s):
    any_spec = pl.BlockSpec(memory_space=pl.ANY)
    dma = lambda *n: pltpu.SemaphoreType.DMA(n)
    nr = len(RELAYED)
    return pl.pallas_call(
        body,
        out_shape=(
            jax.ShapeDtypeStruct((2 * NI, SIDE, SIDE, HC), BF16),
            jax.ShapeDtypeStruct((NI, SIDE, SIDE, C), BF16),
            jax.ShapeDtypeStruct((9, HC, C), F32),
            jax.ShapeDtypeStruct((HC, C), F32),
        ),
        in_specs=[any_spec] * 7,
        out_specs=(any_spec,) * 4,
        scratch_shapes=[
            pltpu.VMEM((NI, PIX, C), BF16),
            pltpu.VMEM((NI, 2, ROWS, HC), BF16),
            pltpu.VMEM((3, 3 * C, C), BF16),
            pltpu.VMEM((3, 3 * C, C), BF16),
            pltpu.VMEM((C, C), BF16),
            pltpu.VMEM((C, C), BF16),
            pltpu.VMEM((NTAP, C, C), F32),
            pltpu.VMEM((NTAP, HC, C), F32),
            pltpu.VMEM((NTAP, HC, C), F32),
            pltpu.VMEM((ROWS + 2 * HALO, 3 * C), BF16),
            pltpu.VMEM((ROWS + 2 * HALO, 3 * C), BF16),
            pltpu.VMEM((ROWS, C), BF16),
            pltpu.VMEM((C, ROWS), BF16),
            pltpu.VMEM((1, C), F32),
            pltpu.VMEM((1, C), F32),
            pltpu.VMEM((1, C), F32),
            pltpu.VMEM((2, SIDE, SIDE, C), BF16),
            pltpu.VMEM((2, 2, SIDE, SIDE, HC), BF16),
            pltpu.VMEM((2, ROWS, HC), BF16),
            pltpu.VMEM((BLK, PBLK), BF16),
            pltpu.VMEM((PBLK, BLK), BF16),
            dma(NI, 2), dma(NI, 2), dma(NI), dma(NI, 2), dma(NI), dma(NI), dma(NTAP), dma(NTAP), dma(NTAP), dma(3), dma(3), dma(3), dma(NI), dma(NI), dma(NI),
            dma(NI, 2, 2), dma(NI, 2, 2), dma(NI), dma(NTAP), dma(NTAP), dma(NTAP, NU), dma(NTAP, NU), dma(nr), dma(nr), dma(nr), dma(nr), dma(NTAP, NU),
        ],
        compiler_params=pltpu.CompilerParams(collective_id=0, has_side_effects=True, vmem_limit_bytes=67043328),
        name="conv_block",
    )(x, dz, w, ws, gamma, beta, gamma_s)


def solution(mesh):
    act_spec = P("stage", ("dp", "tp"), None, None, None)
    kernel_spec = P("stage", None, None, "tp", None)
    short_spec = P("stage", "tp", None)
    vec_spec = P("stage", "tp")
    grad_spec = P("stage", "dp", None, None, "tp")

    def device_step(act_in, w_conv, w_short, gamma, beta, gamma_s, grad_z):
        z, dx, dw, ds = finish(*block(act_in[0], grad_z[0], w_conv.reshape(9, HC, C), w_short[0], gamma, beta, gamma_s))
        return z[None], dx[None], dw.reshape(1, 3, 3, HC, C), ds[None]

    return jax.shard_map(device_step, mesh=mesh, in_specs=(act_spec, kernel_spec, short_spec, vec_spec, vec_spec, vec_spec, grad_spec), out_specs=(grad_spec, act_spec, kernel_spec, short_spec), check_vma=False)
```

```python
import jax
import jax.numpy as jnp
from jax import lax
from jax.experimental import pallas as pl
from jax.experimental.pallas import tpu as pltpu
from jax.sharding import PartitionSpec as P

MESH = pl.DeviceIdType.MESH
F32, BF16 = jnp.float32, jnp.bfloat16
NI = 6
SIDE = 28
PITCH = 32
ROWS = SIDE * PITCH
PIX = SIDE * SIDE
HALO = PITCH
C = 512
HC = 256
BLK, PBLK = 4 * PITCH, 4 * SIDE
CHUNKS = ((0, 512), (512, 384))
DXCHUNKS = ((0, 384), (384, 512))
NTAP = 10
UNIT = 64
RELAYED = tuple((m, s * UNIT, UNIT) for m in range(9) for s in range(2))
STRAIGHT = tuple((m, 2 * UNIT, 2 * UNIT) for m in range(9)) + ((9, 0, 2 * UNIT), (9, 2 * UNIT, 2 * UNIT))
UNITS = RELAYED + STRAIGHT
ARRIVAL = sorted([(2 * i + 2, u) for i, u in enumerate(STRAIGHT)] + [(i + 5.5, u) for i, u in enumerate(RELAYED)])
SPLIT = 5


def rcopy(src, dst, send, recv, dev):
    return pltpu.make_async_remote_copy(src_ref=src, dst_ref=dst, send_sem=send, recv_sem=recv, device_id=dev, device_id_type=MESH)


def dot(a, b):
    return jnp.dot(a, b, preferred_element_type=F32)


def body(x_in, dz_in, w_in, ws_in, gam_in, bet_in, gas_in, z_out, dx_out, dw_out, ds_out,
         xr, dzv, wc, wt, sw, st, acc, tpr, dpr, xcat, gcat, gs, xt, gam, bet, gas, xraw, dzraw, dzt, widen, pack,
         xs, xrv, xl, dzl, dzs, dzr, wl, wsd, wr, vl, vs, vr, zl, zs, zr,
         dxs, dxr, dxo, ts, tr, ys, yr, ras, rar, rbs, rbr, ol):
    tp = lax.axis_index("tp")
    stage = lax.axis_index("stage")
    p_x = {"stage": 1 - stage}
    p_t = {"tp": 1 - tp}
    p_d = {"dp": 1 - lax.axis_index("dp")}

    def load_part(k):
        x_load(k).wait()
        for h in range(SIDE):
            gs[h * PITCH:h * PITCH + SIDE] = xraw[k % 2, h]
        if k + 2 < NI:
            x_load(k + 2).start()

    def pack_part(k, p):
        for b in range(SPLIT) if p == 0 else range(SPLIT, SIDE // 4):
            xr[k, b * PBLK:(b + 1) * PBLK] = dot(pack[...], gs[b * BLK:(b + 1) * BLK]).astype(BF16)

    barrier = pltpu.get_barrier_semaphore()
    for dev in (p_x, p_t, p_d):
        pl.semaphore_signal(barrier, inc=1, device_id=dev, device_id_type=MESH)

    def select(shape, padded_axis):
        wide = lax.broadcasted_iota(jnp.int32, shape, padded_axis)
        slim = lax.broadcasted_iota(jnp.int32, shape, 1 - padded_axis)
        col = wide & (PITCH - 1)
        hit = (slim == (wide >> 5) * SIDE + col) & (col < SIDE)
        return jnp.where(hit, 1.0, 0.0).astype(BF16)


    def x_copy(k, p):
        at = slice(0, SPLIT * PBLK) if p == 0 else slice(SPLIT * PBLK, PIX)
        return rcopy(xr.at[k, at], xr.at[k, at], xs.at[k, p], xrv.at[k, p], p_x)

    def x_load(k):
        return pltpu.make_async_copy(x_in.at[k], xraw.at[k % 2], xl.at[k])

    def dx_copy(k, c, h):
        r, n = DXCHUNKS[c]
        at = slice(r // PITCH * SIDE, (r + n) // PITCH * SIDE)
        return rcopy(xr.at[k, at, h * HC:(h + 1) * HC], dzv.at[k, h, at], dxs.at[k, c, h], dxr.at[k, c, h], p_x)

    def unit_rows(u):
        return pl.ds(pl.multiple_of(tp * HC + u[1], UNIT), u[2])

    def part(ref, u):
        return ref.at[u[0], u[1]:u[1] + u[2]]

    def held(ref, n):
        return part(ref, (n // 4, n % 4 * UNIT, UNIT))

    def relay_a(n):
        u = RELAYED[n]
        return rcopy(acc.at[u[0], unit_rows(u)], held(tpr, n), ys.at[n], rar.at[n], p_x)

    def relay_b(n):
        return rcopy(held(tpr, n), held(dpr, n), ras.at[n], rbr.at[n], p_d)

    def relay_c(n):
        return rcopy(held(dpr, n), part(dpr, RELAYED[n]), rbs.at[n], yr.at[n], p_x)

    widen[...] = select((BLK, PBLK), 0)
    pack[...] = select((PBLK, BLK), 1)

    @pl.when(stage == 0)
    def _():
        x_load(0).start()
        x_load(1).start()
        gs[...] = jnp.zeros((ROWS, C), BF16)
        load_part(0)
        pack_part(0, 0)

    pl.semaphore_wait(barrier, 3)

    @pl.when(stage == 0)
    def _():
        def dx_store(k):
            return pltpu.make_async_copy(xraw.at[k % 2], dx_out.at[k], dxo.at[k])

        x_copy(0, 0).start()
        pack_part(0, 1)
        x_copy(0, 1).start()
        for k in range(1, NI):
            load_part(k)
            pack_part(k, 0)
            if k > 1:
                x_copy(k - 2, 0).wait_send()
                x_copy(k - 2, 1).wait_send()
            x_copy(k, 0).start()
            pack_part(k, 1)
            x_copy(k, 1).start()
        for k in range(NI - 2, NI):
            x_copy(k, 0).wait_send()
            x_copy(k, 1).wait_send()

        def take_dx(k):
            for c in range(2):
                for h in range(2):
                    dx_copy(k, c, h).wait_recv()
            if k > 1:
                dx_store(k - 2).wait()
            for b in range(SIDE // 4):
                for h in range(2):
                    wide = dot(widen[...], dzv[k, h, b * PBLK:(b + 1) * PBLK]).astype(BF16)
                    for r in range(4):
                        xraw[k % 2, 4 * b + r, :, h * HC:(h + 1) * HC] = wide[r * PITCH:r * PITCH + SIDE]
            dx_store(k).start()

        for k in range(NI - 1):
            take_dx(k)
        nr = len(RELAYED)
        for n in range(nr + 1):
            if n < nr:
                relay_a(n).wait_recv()
                relay_b(n).start()
            if n > 0:
                relay_b(n - 1).wait_recv()
                relay_c(n - 1).start()
        take_dx(NI - 1)
        for n in range(nr):
            relay_b(n).wait_send()
            relay_c(n).wait_send()
        dx_store(NI - 2).wait()
        dx_store(NI - 1).wait()

    @pl.when(stage == 1)
    def _():
        lanes = pl.ds(pl.multiple_of(tp * HC, HC), HC)
        other = pl.ds(pl.multiple_of((1 - tp) * HC, HC), HC)

        def dz_load(k, q):
            img = (tp if q == 0 else 1 - tp) * NI + k
            return pltpu.make_async_copy(dz_in.at[img], dzraw.at[lax.rem(k, 2), q], dzl.at[k, q])

        def dz_send(k):
            return rcopy(dzt.at[lax.rem(k, 2)], dzv.at[k, tp], dzs.at[k], dzr.at[k], p_t)

        def w_dst(m):
            if m == 9:
                return sw.at[lanes]
            i, j = divmod(m, 3)
            return wc.at[i, pl.ds(pl.multiple_of(j * C + tp * HC, HC), HC)]

        def w_src(m):
            return ws_in if m == 9 else w_in.at[m]

        def w_local(m):
            return pltpu.make_async_copy(w_src(m), w_dst(m), wl.at[m])

        def w_remote(m):
            return rcopy(w_src(m), w_dst(m), wsd.at[m], wr.at[m], p_t)

        vecs = ((gam_in, gam), (bet_in, bet), (gas_in, gas))

        def v_local(i):
            return pltpu.make_async_copy(vecs[i][0], vecs[i][1].at[:, lanes], vl.at[i])

        def v_remote(i):
            return rcopy(vecs[i][0], vecs[i][1].at[:, lanes], vs.at[i], vr.at[i], p_t)

        def z_local(k):
            return pltpu.make_async_copy(dzraw.at[lax.rem(k, 2), tp], z_out.at[tp * NI + k], zl.at[k])

        def z_remote(k):
            return rcopy(dzraw.at[lax.rem(k, 2), 1 - tp], z_out.at[tp * NI + k], zs.at[k], zr.at[k], p_t)

        def t_copy(m):
            return rcopy(acc.at[m, other], tpr.at[m], ts.at[m], tr.at[m], p_t)

        def y_copy(u):
            n = UNITS.index(u)
            return rcopy(acc.at[u[0], unit_rows(u)], part(dpr, u), ys.at[n], yr.at[n], p_d)

        def out_copy(u):
            rows = slice(u[1], u[1] + u[2])
            dst = ds_out.at[rows] if u[0] == 9 else dw_out.at[u[0], rows]
            return pltpu.make_async_copy(part(tpr, u), dst, ol.at[UNITS.index(u)])

        for k in range(2):
            for q in range(2):
                dz_load(k, q).start()
        for m in range(NTAP):
            w_local(m).start()
            w_remote(m).start()
        for i in range(3):
            v_local(i).start()
            v_remote(i).start()

        zero = jnp.zeros((ROWS, HC), BF16)
        for q in range(2):
            dzt[q] = zero

        @pl.loop(0, NI)
        def _(k):
            dzv[k, tp] = zero
            for q in range(2):
                dz_load(k, q).wait()

            @pl.when(k >= 2)
            def _():
                dz_send(k - 2).wait_send()

            slot = lax.rem(k, 2)
            for h in range(SIDE):
                dzv[k, tp, h * PITCH:h * PITCH + SIDE] = dzraw[slot, 0, h]
                dzt[slot, h * PITCH:h * PITCH + SIDE] = dzraw[slot, 1, h]
            dz_send(k).start()

            @pl.when(k < NI - 2)
            def _():
                for q in range(2):
                    dz_load(k + 2, q).start()

        @pl.loop(0, NTAP)
        def _(m):
            acc[m] = jnp.zeros((C, C), F32)

        for ref in (xcat, gcat):
            ref[0:HALO] = jnp.zeros((HALO, 3 * C), BF16)
            ref[HALO + ROWS:] = jnp.zeros((HALO, 3 * C), BF16)
        for m in range(NTAP):
            w_local(m).wait()
            w_remote(m).wait()
        for i in range(3):
            v_local(i).wait()
            v_remote(i).wait()
        st[...] = sw[...].T

        @pl.loop(0, 3)
        def _(i):
            for j in range(3):
                wt[i, j * C:(j + 1) * C] = wc[i, j * C:(j + 1) * C].T

        @pl.loop(0, 2)
        def _(k):
            dz_send(NI - 2 + k).wait_send()

        def pass_on(m):
            t_copy(m).wait_recv()
            for u in UNITS:
                if u[0] == m:
                    acc[m, unit_rows(u)] = acc[m, unit_rows(u)] + part(tpr, u)[...]
                    relay_a(RELAYED.index(u)).start() if u in RELAYED else y_copy(u).start()

        def forward(k, blocks, r, n):
            for b in blocks:
                xf = dot(widen[...], xr[k, b * PBLK:(b + 1) * PBLK])
                dst = slice(HALO + b * BLK, HALO + (b + 1) * BLK)
                xcat[dst, C:2 * C] = xf.astype(BF16)
                xcat[dst, 0:C] = pltpu.roll(xf, 1, 0).astype(BF16)
                xcat[dst, 2 * C:] = pltpu.roll(xf, BLK - 1, 0).astype(BF16)
            pre = dot(xcat[r:r + n], wc[0]) + dot(xcat[r + HALO:r + HALO + n], wc[1]) + dot(xcat[r + 2 * HALO:r + 2 * HALO + n], wc[2])
            short = dot(xcat[r + HALO:r + HALO + n, C:2 * C], sw[...])
            u = pre * gam[...] + bet[...] + short * gas[...]
            z = jnp.maximum(u, 0.0).astype(BF16)
            for h in range(n // PITCH):
                for q in range(2):
                    dzraw[lax.rem(k, 2), q, r // PITCH + h] = z[h * PITCH:h * PITCH + SIDE, q * HC:(q + 1) * HC]
            dz = jnp.concatenate([dzv[k, 0, r:r + n], dzv[k, 1, r:r + n]], axis=1).astype(F32)
            g = jnp.where(u > 0.0, dz * gam[...], 0.0)
            gs[r:r + n] = jnp.where(u > 0.0, dz * gas[...], 0.0).astype(BF16)
            dst = slice(HALO + r, HALO + r + n)
            gcat[dst, 0:C] = pltpu.roll(g, n - 1, 0).astype(BF16)
            gcat[dst, C:2 * C] = g.astype(BF16)
            gcat[dst, 2 * C:] = pltpu.roll(g, 1, 0).astype(BF16)

        def image(k, last):
            def free_slot():
                z_local(k - 2).wait()
                z_remote(k - 2).wait_send()

            free_slot() if last else pl.when(k >= 2)(free_slot)
            dz_send(k).wait_recv()
            x_copy(k, 0).wait_recv()
            forward(k, range(SPLIT), *CHUNKS[0])

            def input_part(c):
                r, n = DXCHUNKS[c]
                dx = dot(gcat[r + 2 * HALO:r + 2 * HALO + n], wt[0]) + dot(gcat[r + HALO:r + HALO + n], wt[1]) + dot(gcat[r:r + n], wt[2]) + dot(gs[r:r + n], st[...])
                dx = dx.astype(BF16)
                for b in range(n // BLK):
                    at = (r // BLK + b) * PBLK
                    xr[k, at:at + PBLK] = dot(pack[...], dx[b * BLK:(b + 1) * BLK]).astype(BF16)
                for h in range(2):
                    dx_copy(k, c, h).start()

            input_part(0)
            x_copy(k, 1).wait_recv()
            forward(k, range(SPLIT, SIDE // 4), *CHUNKS[1])
            z_local(k).start()
            z_remote(k).start()

            def weight_part():
                xt[...] = xcat[HALO:HALO + ROWS, C:2 * C].T
                for m in range(NTAP):
                    if m == 9:
                        acc[9] += dot(xt[...], gs[...])
                    else:
                        i, j = divmod(m, 3)
                        at = (2 - i) * HALO
                        acc[m] += dot(xt[...], gcat[at:at + ROWS, j * C:(j + 1) * C])
                    if last:
                        t_copy(m).start()
                        if m >= 1:
                            pass_on(m - 1)
                if last:
                    pass_on(NTAP - 1)

            if last:
                weight_part()
                input_part(1)
            else:
                input_part(1)
                weight_part()

        @pl.loop(0, NI - 1)
        def _(k):
            image(k, False)

        image(NI - 1, True)

        for _, u in ARRIVAL:
            y_copy(u).wait_recv()
            tpr[u[0], u[1]:u[1] + u[2]] = acc[u[0], unit_rows(u)] + part(dpr, u)[...]
            out_copy(u).start()

        for m in range(NTAP):
            t_copy(m).wait_send()
        for u in UNITS:
            y_copy(u).wait_send()
            out_copy(u).wait()

        for k in range(NI - 2, NI):
            z_local(k).wait()
            z_remote(k).wait_send()
        for k in range(NI):
            z_remote(k).wait_recv()
            for c in range(2):
                for h in range(2):
                    dx_copy(k, c, h).wait_send()


def finish_body(z_in, dx_in, dw_in, ds_in, z_out, dx_out, dw_out, ds_out, zb, dxb, dwb, dsb, z0, dx0, dw0, sems):
    stage = lax.axis_index("stage")
    groups = ((z_in, zb, z_out, z0, 2 * NI, 1), (dx_in, dxb, dx_out, dx0, NI, 0), (dw_in, dwb, dw_out, dw0, 9, 1), (ds_in, dsb, ds_out, dw0, 1, 1))

    def run(here):
        def pick(ref, k):
            return ref.at[k] if len(ref.shape) > 2 else ref

        ins, outs, n = [], [], 0
        for src, buf, dst, nil, count, owner in groups:
            for k in range(count):
                if owner == here:
                    ins.append(pltpu.make_async_copy(pick(src, k), pick(buf, k), sems.at[0, n]))
                    outs.append(pltpu.make_async_copy(pick(buf, k), pick(dst, k), sems.at[1, n]))
                else:
                    outs.append(pltpu.make_async_copy(nil, pick(dst, k), sems.at[1, n]))
                    ins.append(None)
                n += 1
        for c in ins:
            if c is not None:
                c.start()
        if here == 0:
            z0[...] = jnp.zeros(z0.shape, z0.dtype)
            dw0[...] = jnp.zeros(dw0.shape, dw0.dtype)
        else:
            dx0[...] = jnp.zeros(dx0.shape, dx0.dtype)
        for c, o in zip(ins, outs):
            if c is None:
                o.start()
        for c, o in zip(ins, outs):
            if c is not None:
                c.wait()
                o.start()
        for o in outs:
            o.wait()

    for here in range(2):
        pl.when(stage == here)(lambda here=here: run(here))


def finish(z, dx, dw, ds):
    any_spec = pl.BlockSpec(memory_space=pl.ANY)
    total = 2 * NI + NI + 9 + 1
    return pl.pallas_call(
        finish_body,
        out_shape=tuple(jax.ShapeDtypeStruct(a.shape, a.dtype) for a in (z, dx, dw, ds)),
        in_specs=[any_spec] * 4,
        out_specs=(any_spec,) * 4,
        scratch_shapes=[pltpu.VMEM(a.shape, a.dtype) for a in (z, dx, dw, ds)]
        + [pltpu.VMEM(z.shape[1:], z.dtype), pltpu.VMEM(dx.shape[1:], dx.dtype), pltpu.VMEM(ds.shape, ds.dtype), pltpu.SemaphoreType.DMA((2, total))],
        compiler_params=pltpu.CompilerParams(vmem_limit_bytes=67043328),
        name="finish",
    )(z, dx, dw, ds)


def block(x, dz, w, ws, gamma, beta, gamma_s):
    any_spec = pl.BlockSpec(memory_space=pl.ANY)
    dma = lambda *n: pltpu.SemaphoreType.DMA(n)
    nr = len(RELAYED)
    return pl.pallas_call(
        body,
        out_shape=(
            jax.ShapeDtypeStruct((2 * NI, SIDE, SIDE, HC), BF16),
            jax.ShapeDtypeStruct((NI, SIDE, SIDE, C), BF16),
            jax.ShapeDtypeStruct((9, HC, C), F32),
            jax.ShapeDtypeStruct((HC, C), F32),
        ),
        in_specs=[any_spec] * 7,
        out_specs=(any_spec,) * 4,
        scratch_shapes=[
            pltpu.VMEM((NI, PIX, C), BF16),
            pltpu.VMEM((NI, 2, ROWS, HC), BF16),
            pltpu.VMEM((3, 3 * C, C), BF16),
            pltpu.VMEM((3, 3 * C, C), BF16),
            pltpu.VMEM((C, C), BF16),
            pltpu.VMEM((C, C), BF16),
            pltpu.VMEM((NTAP, C, C), F32),
            pltpu.VMEM((NTAP, HC, C), F32),
            pltpu.VMEM((NTAP, HC, C), F32),
            pltpu.VMEM((ROWS + 2 * HALO, 3 * C), BF16),
            pltpu.VMEM((ROWS + 2 * HALO, 3 * C), BF16),
            pltpu.VMEM((ROWS, C), BF16),
            pltpu.VMEM((C, ROWS), BF16),
            pltpu.VMEM((1, C), F32),
            pltpu.VMEM((1, C), F32),
            pltpu.VMEM((1, C), F32),
            pltpu.VMEM((2, SIDE, SIDE, C), BF16),
            pltpu.VMEM((2, 2, SIDE, SIDE, HC), BF16),
            pltpu.VMEM((2, ROWS, HC), BF16),
            pltpu.VMEM((BLK, PBLK), BF16),
            pltpu.VMEM((PBLK, BLK), BF16),
            dma(NI, 2), dma(NI, 2), dma(NI), dma(NI, 2), dma(NI), dma(NI), dma(NTAP), dma(NTAP), dma(NTAP), dma(3), dma(3), dma(3), dma(NI), dma(NI), dma(NI),
            dma(NI, 2, 2), dma(NI, 2, 2), dma(NI), dma(NTAP), dma(NTAP), dma(len(UNITS)), dma(len(UNITS)), dma(nr), dma(nr), dma(nr), dma(nr), dma(len(UNITS)),
        ],
        compiler_params=pltpu.CompilerParams(collective_id=0, has_side_effects=True, vmem_limit_bytes=67043328),
        name="conv_block",
    )(x, dz, w, ws, gamma, beta, gamma_s)


def solution(mesh):
    act_spec = P("stage", ("dp", "tp"), None, None, None)
    kernel_spec = P("stage", None, None, "tp", None)
    short_spec = P("stage", "tp", None)
    vec_spec = P("stage", "tp")
    grad_spec = P("stage", "dp", None, None, "tp")

    def device_step(act_in, w_conv, w_short, gamma, beta, gamma_s, grad_z):
        z, dx, dw, ds = finish(*block(act_in[0], grad_z[0], w_conv.reshape(9, HC, C), w_short[0], gamma, beta, gamma_s))
        return z[None], dx[None], dw.reshape(1, 3, 3, HC, C), ds[None]

    return jax.shard_map(device_step, mesh=mesh, in_specs=(act_spec, kernel_spec, short_spec, vec_spec, vec_spec, vec_spec, grad_spec), out_specs=(grad_spec, act_spec, kernel_spec, short_spec), check_vma=False)
```
